32 devices in a mesh: lat: 16 (over z, x, core), tm: 2 (over y).
Axes of the slice: x: 2, y: 2, z: 4, core: 2. Of those that a mesh axis runs over, the one named last changes fastest.
Arguments:
- fields: bfloat16 [512, 64, 1024], P('lat', 'tm'), may hold values from -16 to 16
Outputs:
- covariance: float32 [64, 64], P('tm')
The draws below stay inside these ranges and needn't reach their ends.
All inputs are finite; a program needn't handle non-finite values.
Results may differ from the reference program's by a relative error of at most 0.0003.
Values may be sent and summed in bfloat16 or wider, within the bound.
A program may use at most 64 MiB of HBM per device.

```python
import math
import jax
import jax.numpy as jnp
from jax import lax

NLON = 1024
NLAT = 512
TRUNC = 341
MSLOT = 384
DSLOT = 384
MONTHS = 64


def draw_fields(key, part):
    patterns_count = 8
    half_lon = NLON // 2
    waves = jnp.arange(half_lon).astype(jnp.int32)
    longitude = jnp.arange(NLON).astype(jnp.int32)
    phase = 2.0 * math.pi * (waves[:, None] * longitude[None, :] % NLON).astype(jnp.float32) / NLON
    redness = 1.0 / (1.0 + waves.astype(jnp.float32) / (NLON / 2.0))
    cos_amps = jax.random.normal(jax.random.fold_in(key, 1), (patterns_count * NLAT, half_lon), jnp.float32) * redness
    sin_amps = jax.random.normal(jax.random.fold_in(key, 2), (patterns_count * NLAT, half_lon), jnp.float32) * redness
    patterns = jnp.dot(cos_amps, jnp.cos(phase)) + jnp.dot(sin_amps, jnp.sin(phase))
    patterns = patterns / jnp.sqrt(jnp.mean(patterns * patterns) + 1e-06)
    patterns = patterns.reshape(patterns_count, NLAT, NLON)
    month_amps = jax.random.normal(jax.random.fold_in(key, 3), (MONTHS, patterns_count), jnp.float32) / math.sqrt(patterns_count)
    month_scale = 1.0 + 2.0 * jnp.arange(MONTHS).astype(jnp.float32) / max(MONTHS - 1, 1)
    shared = jnp.einsum('tk,kjl->jtl', month_amps, patterns)
    noise = 0.5 * jax.random.normal(jax.random.fold_in(key, 4), (NLAT, MONTHS, NLON), jnp.float32)
    values = month_scale[None, :, None] * (shared + noise)
    return jnp.clip(values, -16.0, 16.0).astype(jnp.bfloat16)


def setup_inputs(seed: int = 0) -> dict:
    key_of = jax.random.split(jax.random.key(seed), 2)
    fields = draw_fields(jax.random.fold_in(key_of[1], 71), 0)
    return dict(fields=fields)


def start_value(order, sine_lat):
    log_start = 0.5 * (math.log(0.5) + lax.lgamma(order + 1.5) - (0.5 * math.log(math.pi) - math.log(2.0)) - lax.lgamma(order + 1.0)) + order * jnp.log(sine_lat)
    taper = jnp.clip((log_start + 70.0) / 10.0, 0.0, 1.0)
    return jnp.exp(jnp.maximum(log_start, -80.0)) * taper

def step_factors(order, degree):
    top = jnp.sqrt((4.0 * degree * degree - 1.0) / (degree * degree - order * order))
    below = degree - 1.0
    back = jnp.sqrt(jnp.maximum(below * below - order * order, 0.0) / jnp.abs(4.0 * below * below - 1.0))
    return (top, top * back)

def legendre_column(order, cosine_lat, sine_lat):
    first = start_value(order, sine_lat)

    def advance(carry, offset):
        current, previous = carry
        top, mixed = step_factors(order, order + offset)
        following = top * cosine_lat * current - mixed * previous
        return ((following, current), following)
    offsets = jnp.arange(1, DSLOT).astype(jnp.float32)
    _, later = lax.scan(advance, (first, jnp.zeros_like(first)), offsets)
    return jnp.concatenate([first[None, :], later], axis=0)

def weighted_basis(order, cosine_lat, sine_lat, weight):
    values = legendre_column(order, cosine_lat, sine_lat)
    offsets = jnp.arange(DSLOT).astype(jnp.float32)
    keep = (order + offsets <= TRUNC).astype(jnp.float32)
    factor = jnp.where(order > 0, math.sqrt(2.0), 1.0)
    table = values * keep[:, None] * weight[None, :] * factor
    return table.T.astype(jnp.bfloat16)

def reference(fields):
    longitude = jnp.arange(NLON).astype(jnp.int32)
    waves = jnp.arange(MSLOT).astype(jnp.int32)
    phase = 2.0 * math.pi * (longitude[:, None] * waves[None, :] % NLON).astype(jnp.float32) / NLON
    keep = (waves <= TRUNC).astype(jnp.float32)
    table = jnp.stack([jnp.cos(phase), -jnp.sin(phase)], axis=-1) * keep[None, :, None] / math.sqrt(NLON)
    table = table.reshape(NLON, 2 * MSLOT).astype(jnp.bfloat16)

    def per_row(row_fields):
        return jnp.dot(row_fields, table, preferred_element_type=jnp.float32).astype(jnp.bfloat16)
    fourier = lax.map(per_row, fields)
    fourier = fourier.reshape(NLAT, MONTHS, MSLOT, 2).transpose(2, 0, 1, 3)
    theta = math.pi * (jnp.arange(NLAT).astype(jnp.float32) + 0.5) / NLAT
    cosine_lat = jnp.cos(theta)
    sine_lat = jnp.sin(theta)
    weight = math.pi * sine_lat / NLAT

    def accumulate(gram, inputs):
        order_index, block = inputs
        order = order_index.astype(jnp.float32)
        basis = weighted_basis(order, cosine_lat, sine_lat, weight)
        coefficients = jnp.dot(block.reshape(NLAT, MONTHS * 2).T, basis, preferred_element_type=jnp.float32)
        coefficients = coefficients.astype(jnp.bfloat16).reshape(MONTHS, 2 * DSLOT)
        gram = gram + jnp.dot(coefficients, coefficients.T, preferred_element_type=jnp.float32)
        return (gram, None)
    gram, _ = lax.scan(accumulate, jnp.zeros((MONTHS, MONTHS), jnp.float32), (jnp.arange(MSLOT).astype(jnp.int32), fourier))
    trace = jnp.sum(jnp.diagonal(gram))
    return MONTHS * gram / (trace + 1e-06)
```

```python
import functools
import math

import jax
import jax.numpy as jnp
import numpy as np
from jax import lax
from jax.experimental import pallas as pl
from jax.experimental.pallas import tpu as pltpu
from jax.sharding import PartitionSpec as P

TRUNC = 341
GROUP = 8
LANES = 128
HALF = 64
PIECE = 8
MESH = pl.DeviceIdType.MESH


def twiddle_table(device_total, slots, lon_count):
    groups = device_total // GROUP
    device = np.arange(device_total).reshape(groups, 1, GROUP, 1)
    slot = np.arange(slots).reshape(1, 1, 1, slots)
    wave = np.broadcast_to(slot * device_total + device, (groups, 1, GROUP, slots))
    longitude = np.arange(lon_count)
    phase = 2.0 * math.pi * ((wave[..., None] * longitude) % lon_count) / lon_count
    table = np.concatenate([np.cos(phase), -np.sin(phase)], axis=1)
    table = table * (wave[..., None] <= TRUNC) / math.sqrt(lon_count)
    table = table.reshape(groups, 2 * GROUP * slots, lon_count)
    return table.astype(np.float32).astype(jnp.bfloat16)


def start_table(device_total, slots, slot_rows):
    table = np.zeros((device_total, slot_rows), np.float64)
    for device in range(device_total):
        for slot in range(slot_rows):
            order = min(slot, slots - 1) * device_total + device
            table[device, slot] = 0.5 * (
                math.log(0.5)
                + math.lgamma(order + 1.5)
                - math.lgamma(1.5)
                - math.lgamma(order + 1.0)
            )
    table = np.broadcast_to(table[:, :, None], (device_total, slot_rows, LANES))
    return table.astype(np.float32)


def lat_table(lat_total, share):
    lat = np.arange(lat_total).reshape(lat_total // share, share).T.reshape(-1)
    theta = math.pi * (lat + 0.5) / lat_total
    table = np.stack([np.cos(theta), np.log(np.sin(theta)), math.pi * np.sin(theta) / lat_total])
    return table.reshape(3, lat_total // LANES, LANES).astype(np.float32)


def kernel(
    dims,
    x_ref,
    table_ref,
    start_ref,
    lat_ref,
    out_ref,
    spread,
    outbox,
    inbox,
    legendre,
    gram_ref,
    local_gram,
    parts,
    own_sum,
    full,
    send_sem,
    recv_sem,
    part_send,
    part_recv,
    sum_send,
    sum_recv,
):
    lat_devices, tm_devices, rows, months, lon_count, slots, slot_rows, depth = dims
    device_total = lat_devices * tm_devices
    groups = device_total // GROUP
    share = HALF // months
    high = rows // share
    lat_total = lat_devices * rows
    lat_groups = lat_total // LANES
    month_total = months * tm_devices
    pieces = month_total // PIECE
    stride = device_total // pieces
    lat_me = lax.axis_index("lat")
    tm_me = lax.axis_index("tm")
    me = lat_me * tm_devices + tm_me

    def coords(device):
        return (device // tm_devices, lax.rem(device, tm_devices))

    barrier = pltpu.get_barrier_semaphore()

    @pl.loop(1, device_total)
    def _(step):
        pl.semaphore_signal(
            barrier,
            inc=1,
            device_id=coords(lax.rem(me + step, device_total)),
            device_id_type=MESH,
        )

    group_rows = GROUP * slots
    lane = lax.broadcasted_iota(jnp.int32, (group_rows, LANES), 1)
    lower = lane < HALF

    @pl.loop(0, groups)
    def _(group):
        values = lax.dot_general(
            table_ref[group],
            x_ref[...],
            (((1,), (1,)), ((), ())),
            preferred_element_type=jnp.float32,
        )
        for block in range(rows * months // LANES):
            cosine = values[:group_rows, block * LANES : (block + 1) * LANES]
            sine = values[group_rows:, block * LANES : (block + 1) * LANES]
            even = jnp.where(lower, cosine, pltpu.roll(sine, HALF, 1))
            odd = jnp.where(lower, pltpu.roll(cosine, HALF, 1), sine)
            spread[pl.ds(2 * block, group_rows, stride=high), :] = even
            spread[pl.ds(2 * block + 1, group_rows, stride=high), :] = odd
        packed = spread[...].astype(jnp.bfloat16)
        outbox[pl.ds(group * GROUP, GROUP)] = packed.reshape(GROUP, slots, high, LANES)

    pl.semaphore_wait(barrier, device_total - 1)

    def exchange(target, source):
        return pltpu.make_async_remote_copy(
            src_ref=outbox.at[target],
            dst_ref=inbox.at[source],
            send_sem=send_sem.at[target],
            recv_sem=recv_sem.at[source],
            device_id=coords(target),
            device_id_type=MESH,
        )

    @pl.loop(1, device_total)
    def _(step):
        exchange(lax.rem(me + step, device_total), me).start()

    inbox[me] = outbox[me]

    halves = slot_rows // 8
    sub = lax.broadcasted_iota(jnp.int32, (8, LANES), 0)
    slot_of = [sub + 8 * half for half in range(halves)]
    order_int = [slot * device_total + me for slot in slot_of]
    order = [value.astype(jnp.float32) for value in order_int]
    cosine_lat = [jnp.broadcast_to(lat_ref[0, pl.ds(g, 1), :], (8, LANES)) for g in range(lat_groups)]
    current = []
    scale = []
    for half in range(halves):
        factor = jnp.where(order_int[half] > 0, math.sqrt(2.0), 1.0)
        for g in range(lat_groups):
            log_start = (
                start_ref[me, pl.ds(8 * half, 8), :]
                + order[half] * jnp.broadcast_to(lat_ref[1, pl.ds(g, 1), :], (8, LANES))
            )
            taper = jnp.clip((log_start + 70.0) / 10.0, 0.0, 1.0)
            current.append(jnp.exp(jnp.maximum(log_start, -80.0)) * taper)
            scale.append(factor * jnp.broadcast_to(lat_ref[2, pl.ds(g, 1), :], (8, LANES)))

    def store(offset, values):
        for half in range(halves):
            keep = (order_int[half] + offset <= TRUNC) & (slot_of[half] < slots)
            for g in range(lat_groups):
                index = half * lat_groups + g
                value = jnp.where(keep, values[index] * scale[index], 0.0)
                legendre[g, pl.ds(8 * half * depth + offset, 8, stride=depth), :] = value

    store(0, current)

    def advance(offset, carry):
        now, before, backs = carry
        real = lax.convert_element_type(offset, jnp.float32)
        following = []
        next_backs = []
        for half in range(halves):
            degree = order[half] + real
            ratio = (4.0 * degree * degree - 1.0) / (real * (order[half] + degree))
            top = jnp.sqrt(ratio)
            next_backs.append(1.0 / top)
            for g in range(lat_groups):
                index = half * lat_groups + g
                following.append(
                    top * (cosine_lat[g] * now[index] - backs[half] * before[index])
                )
        store(offset, following)
        return following, now, next_backs

    zero = jnp.zeros((8, LANES), jnp.float32)
    lax.fori_loop(
        1,
        depth,
        advance,
        (current, [zero] * len(current), [zero] * halves),
        unroll=7,
    )

    @pl.loop(1, device_total)
    def _(step):
        source = lax.rem(me + step, device_total)
        exchange(source, source).wait_recv()

    per_share = lat_groups // share
    width = tm_devices * LANES
    share_of = lax.broadcasted_iota(jnp.int32, (depth, width), 1) % HALF // months
    gram_ref[...] = jnp.zeros_like(gram_ref)

    @pl.loop(0, slots)
    def _(slot):
        received = jnp.concatenate(
            [
                jnp.concatenate(
                    [
                        inbox[lat_device * tm_devices + tm, slot]
                        for lat_device in range(lat_devices)
                    ],
                    axis=0,
                )
                for tm in range(tm_devices)
            ],
            axis=1,
        )
        first = pl.multiple_of(slot * depth, 8)
        merged = None
        for part in range(share):
            basis = jnp.concatenate(
                [
                    legendre[part * per_share + g, pl.ds(first, depth), :].astype(jnp.bfloat16)
                    for g in range(per_share)
                ],
                axis=1,
            )
            product = jnp.dot(basis, received, preferred_element_type=jnp.float32)
            merged = product if part == 0 else jnp.where(share_of == part, product, merged)
        total = merged
        for part in range(1, share):
            total = total + pltpu.roll(merged, width - part * months, 1)
        coefficients = jnp.where(share_of == 0, total, 0.0).astype(jnp.bfloat16)
        gram_ref[...] += lax.dot_general(
            coefficients,
            coefficients,
            (((0,), (0,)), ((), ())),
            preferred_element_type=jnp.float32,
        )

    gram = None
    for part in range(2):
        across = jnp.concatenate(
            [
                gram_ref[pl.ds(tm * LANES + part * HALF, months), :]
                for tm in range(tm_devices)
            ],
            axis=0,
        )
        block = jnp.concatenate(
            [
                across[:, tm * LANES + part * HALF : tm * LANES + part * HALF + months]
                for tm in range(tm_devices)
            ],
            axis=1,
        )
        gram = block if gram is None else gram + block
    local_gram[...] = gram.reshape(pieces, PIECE, month_total)

    def owner(piece):
        return piece * stride + stride // 2

    def send_part(piece, source):
        return pltpu.make_async_remote_copy(
            src_ref=local_gram.at[piece],
            dst_ref=parts.at[source],
            send_sem=part_send.at[piece],
            recv_sem=part_recv.at[source],
            device_id=coords(owner(piece)),
            device_id_type=MESH,
        )

    def send_sum(piece, target):
        return pltpu.make_async_remote_copy(
            src_ref=own_sum,
            dst_ref=full.at[piece],
            send_sem=sum_send.at[target],
            recv_sem=sum_recv.at[piece],
            device_id=coords(target),
            device_id_type=MESH,
        )

    @pl.loop(0, pieces)
    def _(piece):
        @pl.when(owner(piece) != me)
        def _():
            send_part(piece, me).start()

    my_piece = me // stride

    @pl.when(lax.rem(me, stride) == stride // 2)
    def _():
        parts[me] = local_gram[my_piece]

        @pl.loop(1, device_total)
        def _(step):
            source = lax.rem(me + step, device_total)
            send_part(my_piece, source).wait_recv()

        total = lax.fori_loop(
            0,
            device_total,
            lambda source, value: value + parts[source],
            jnp.zeros((PIECE, month_total), jnp.float32),
        )
        own_sum[...] = total
        full[my_piece] = total

        @pl.loop(1, device_total)
        def _(step):
            send_sum(my_piece, lax.rem(me + step, device_total)).start()

    @pl.loop(0, pieces)
    def _(piece):
        @pl.when(owner(piece) != me)
        def _():
            send_sum(piece, me).wait_recv()

    gram = full[...].reshape(month_total, month_total)
    on_diagonal = lax.broadcasted_iota(jnp.int32, gram.shape, 0) == lax.broadcasted_iota(
        jnp.int32, gram.shape, 1
    )
    trace = jnp.sum(jnp.where(on_diagonal, gram, 0.0))
    mine = full[pl.ds(tm_me * (months // PIECE), months // PIECE)].reshape(months, month_total)
    out_ref[...] = month_total * mine / (trace + 1e-06)

    @pl.loop(1, device_total)
    def _(step):
        exchange(lax.rem(me + step, device_total), me).wait_send()

    @pl.loop(0, pieces)
    def _(piece):
        @pl.when(owner(piece) != me)
        def _():
            send_part(piece, me).wait_send()

    @pl.when(lax.rem(me, stride) == stride // 2)
    def _():
        @pl.loop(1, device_total)
        def _(step):
            send_sum(my_piece, lax.rem(me + step, device_total)).wait_send()


def solution(mesh):
    lat_devices = mesh.shape["lat"]
    tm_devices = mesh.shape["tm"]
    device_total = lat_devices * tm_devices
    slots = -(-(TRUNC + 1) // device_total)
    slot_rows = -(-slots // 8) * 8
    depth = -(-(TRUNC + 1) // 8) * 8

    def local(fields):
        rows, months, lon_count = fields.shape
        month_total = months * tm_devices
        lat_total = rows * lat_devices
        share = HALF // months
        high = rows // share
        pieces = month_total // PIECE
        width = tm_devices * LANES
        dims = (lat_devices, tm_devices, rows, months, lon_count, slots, slot_rows, depth)
        table = jnp.asarray(twiddle_table(device_total, slots, lon_count))
        starts = jnp.asarray(start_table(device_total, slots, slot_rows))
        lats = jnp.asarray(lat_table(lat_total, share))
        vmem = pl.BlockSpec(memory_space=pltpu.VMEM)
        dma = pltpu.SemaphoreType.DMA
        return pl.pallas_call(
            functools.partial(kernel, dims),
            out_shape=jax.ShapeDtypeStruct((months, month_total), jnp.float32),
            in_specs=[vmem] * 4,
            out_specs=vmem,
            scratch_shapes=[
                pltpu.VMEM((GROUP * slots * high, LANES), jnp.float32),
                pltpu.VMEM((device_total, slots, high, LANES), jnp.bfloat16),
                pltpu.VMEM((device_total, slots, high, LANES), jnp.bfloat16),
                pltpu.VMEM((lat_total // LANES, slot_rows * depth, LANES), jnp.float32),
                pltpu.VMEM((width, width), jnp.float32),
                pltpu.VMEM((pieces, PIECE, month_total), jnp.float32),
                pltpu.VMEM((device_total, PIECE, month_total), jnp.float32),
                pltpu.VMEM((PIECE, month_total), jnp.float32),
                pltpu.VMEM((pieces, PIECE, month_total), jnp.float32),
                dma((device_total,)),
                dma((device_total,)),
                dma((pieces,)),
                dma((device_total,)),
                dma((device_total,)),
                dma((pieces,)),
            ],
            compiler_params=pltpu.CompilerParams(
                collective_id=0, has_side_effects=True, vmem_limit_bytes=60 * 1024 * 1024
            ),
        )(fields.reshape(rows * months, lon_count), table, starts, lats)

    return jax.shard_map(
        local, mesh=mesh, in_specs=(P("lat", "tm", None),), out_specs=P("tm", None), check_vma=False
    )
```

```python
import functools
import math

import jax
import jax.numpy as jnp
import numpy as np
from jax import lax
from jax.experimental import pallas as pl
from jax.experimental.pallas import tpu as pltpu
from jax.sharding import PartitionSpec as P

TRUNC = 341
GROUP = 8
LANES = 128
HALF = 64
PIECE = 8
PHASES = 4
MESH = pl.DeviceIdType.MESH


def twiddle_table(device_total, slots, lon_count):
    groups = device_total // GROUP
    device = np.arange(device_total).reshape(groups, 1, GROUP, 1)
    slot = np.arange(slots).reshape(1, 1, 1, slots)
    wave = np.broadcast_to(slot * device_total + device, (groups, 1, GROUP, slots))
    longitude = np.arange(lon_count)
    phase = 2.0 * math.pi * ((wave[..., None] * longitude) % lon_count) / lon_count
    table = np.concatenate([np.cos(phase), -np.sin(phase)], axis=1)
    table = table * (wave[..., None] <= TRUNC) / math.sqrt(lon_count)
    table = table.reshape(groups, 2 * GROUP * slots, lon_count)
    return table.astype(np.float32).astype(jnp.bfloat16)


def start_table(device_total, slots, slot_rows):
    table = np.zeros((device_total, slot_rows), np.float64)
    for device in range(device_total):
        for slot in range(slot_rows):
            order = min(slot, slots - 1) * device_total + device
            table[device, slot] = 0.5 * (
                math.log(0.5)
                + math.lgamma(order + 1.5)
                - math.lgamma(1.5)
                - math.lgamma(order + 1.0)
            )
    table = np.broadcast_to(table[:, :, None], (device_total, slot_rows, LANES))
    return table.astype(np.float32)


def needed_slots(lat_devices, device_total, slots, rows):
    counts = []
    order = np.arange(slots * device_total)
    rise = np.array(
        [math.lgamma(m + 1.5) - math.lgamma(1.5) - math.lgamma(m + 1.0) for m in order]
    )
    for device in range(lat_devices):
        lat = device * rows + np.arange(rows)
        sine = np.sin(math.pi * (lat + 0.5) / (lat_devices * rows))
        start = 0.5 * (math.log(0.5) + rise[:, None]) + order[:, None] * np.log(sine)[None, :]
        used = (start > -70.5) & (order <= TRUNC)[:, None]
        used = used.reshape(slots, -1).any(axis=1)
        counts.append(int(np.max(np.nonzero(used)[0])) + 1 if used.any() else 0)
    runs = []
    for device, count in enumerate(counts):
        if runs and runs[-1][2] == count:
            runs[-1][1] = device + 1
        else:
            runs.append([device, device + 1, count])
    return tuple(tuple(run) for run in runs)


def lat_table(lat_total, share):
    lat = np.arange(lat_total).reshape(lat_total // share, share).T.reshape(-1)
    theta = math.pi * (lat + 0.5) / lat_total
    table = np.stack([np.cos(theta), np.log(np.sin(theta)), math.pi * np.sin(theta) / lat_total])
    return table.reshape(3, lat_total // LANES, LANES).astype(np.float32)


def kernel(
    dims,
    runs,
    x_hbm,
    table_hbm,
    start_ref,
    lat_ref,
    out_ref,
    x_ref,
    table_ref,
    spread,
    outbox,
    inbox,
    legendre,
    gram_ref,
    local_gram,
    parts,
    own_sum,
    full,
    x_sem,
    table_sem,
    send_sem,
    recv_sem,
    part_send,
    part_recv,
    sum_send,
    sum_recv,
):
    lat_devices, tm_devices, rows, months, lon_count, slots, slot_rows, depth = dims
    device_total = lat_devices * tm_devices
    groups = device_total // GROUP
    share = HALF // months
    high = rows // share
    lat_total = lat_devices * rows
    lat_groups = lat_total // LANES
    month_total = months * tm_devices
    pieces = month_total // PIECE
    stride = device_total // 2 // pieces
    first_owner = device_total // 4
    lat_me = lax.axis_index("lat")
    tm_me = lax.axis_index("tm")
    me = lat_me * tm_devices + tm_me

    def coords(device):
        return (device // tm_devices, lax.rem(device, tm_devices))

    x_copy = pltpu.make_async_copy(x_hbm, x_ref, x_sem)
    x_copy.start()

    def table_copy(group):
        return pltpu.make_async_copy(
            table_hbm.at[group], table_ref.at[group], table_sem.at[group]
        )

    @pl.loop(0, groups)
    def _(group):
        table_copy(group).start()

    barrier = pltpu.get_barrier_semaphore()

    @pl.loop(1, device_total)
    def _(step):
        pl.semaphore_signal(
            barrier,
            inc=1,
            device_id=coords(lax.rem(me + step, device_total)),
            device_id_type=MESH,
        )

    group_rows = GROUP * slots
    lane = lax.broadcasted_iota(jnp.int32, (group_rows, LANES), 1)
    lower = lane < HALF

    for first, last, count in runs:
        if count < slots:

            @pl.loop(first * tm_devices, last * tm_devices)
            def _(source):
                inbox[source, count:] = jnp.zeros((slots - count, high, LANES), jnp.bfloat16)

    x_copy.wait()

    @pl.loop(0, groups)
    def _(group):
        table_copy(group).wait()
        values = lax.dot_general(
            table_ref[group],
            x_ref[...],
            (((1,), (1,)), ((), ())),
            preferred_element_type=jnp.float32,
        )
        for block in range(rows * months // LANES):
            cosine = values[:group_rows, block * LANES : (block + 1) * LANES]
            sine = values[group_rows:, block * LANES : (block + 1) * LANES]
            even = jnp.where(lower, cosine, pltpu.roll(sine, HALF, 1))
            odd = jnp.where(lower, pltpu.roll(cosine, HALF, 1), sine)
            spread[pl.ds(2 * block, group_rows, stride=high), :] = even
            spread[pl.ds(2 * block + 1, group_rows, stride=high), :] = odd
        packed = spread[...].astype(jnp.bfloat16)
        outbox[pl.ds(group * GROUP, GROUP)] = packed.reshape(GROUP, slots, high, LANES)

    pl.semaphore_wait(barrier, device_total - 1)

    phase_length = -(-slots // PHASES)
    phases = [(low, min(low + phase_length, slots)) for low in range(0, slots, phase_length)]

    def exchange(phase, count, target, source):
        low, top = phases[phase]
        span = pl.ds(low, min(count, top) - low)
        return pltpu.make_async_remote_copy(
            src_ref=outbox.at[target, span],
            dst_ref=inbox.at[source, span],
            send_sem=send_sem.at[phase, target],
            recv_sem=recv_sem.at[phase, source],
            device_id=coords(target),
            device_id_type=MESH,
        )

    def each_send(act):
        for phase in range(len(phases)):
            for first, last, count in runs:
                if count > phases[phase][0]:

                    @pl.when((lat_me >= first) & (lat_me < last))
                    def _():
                        @pl.loop(1, device_total)
                        def _(step):
                            act(exchange(phase, count, lax.rem(me + step, device_total), me))

    each_send(lambda copy: copy.start())

    inbox[me] = outbox[me]

    halves = slot_rows // 8
    sub = lax.broadcasted_iota(jnp.int32, (8, LANES), 0)
    slot_of = [sub + 8 * half for half in range(halves)]
    order_int = [slot * device_total + me for slot in slot_of]
    order = [value.astype(jnp.float32) for value in order_int]
    cosine_lat = [jnp.broadcast_to(lat_ref[0, pl.ds(g, 1), :], (8, LANES)) for g in range(lat_groups)]
    current = []
    scale = []
    for half in range(halves):
        factor = jnp.where(order_int[half] > 0, math.sqrt(2.0), 1.0)
        for g in range(lat_groups):
            log_start = (
                start_ref[me, pl.ds(8 * half, 8), :]
                + order[half] * jnp.broadcast_to(lat_ref[1, pl.ds(g, 1), :], (8, LANES))
            )
            taper = jnp.clip((log_start + 70.0) / 10.0, 0.0, 1.0)
            current.append(jnp.exp(jnp.maximum(log_start, -80.0)) * taper)
            scale.append(factor * jnp.broadcast_to(lat_ref[2, pl.ds(g, 1), :], (8, LANES)))

    def store(offset, values):
        for half in range(halves):
            keep = (order_int[half] + offset <= TRUNC) & (slot_of[half] < slots)
            for g in range(lat_groups):
                index = half * lat_groups + g
                value = jnp.where(keep, values[index] * scale[index], 0.0)
                legendre[g, pl.ds(8 * half * depth + offset, 8, stride=depth), :] = value

    store(0, current)

    def advance(offset, carry):
        now, before, backs = carry
        real = lax.convert_element_type(offset, jnp.float32)
        following = []
        next_backs = []
        for half in range(halves):
            degree = order[half] + real
            ratio = (4.0 * degree * degree - 1.0) / (real * (order[half] + degree))
            top = jnp.sqrt(ratio)
            next_backs.append(1.0 / top)
            for g in range(lat_groups):
                index = half * lat_groups + g
                following.append(
                    top * (cosine_lat[g] * now[index] - backs[half] * before[index])
                )
        store(offset, following)
        return following, now, next_backs

    zero = jnp.zeros((8, LANES), jnp.float32)
    lax.fori_loop(
        1,
        depth,
        advance,
        (current, [zero] * len(current), [zero] * halves),
        unroll=7,
    )

    per_share = lat_groups // share
    width = tm_devices * LANES
    share_of = lax.broadcasted_iota(jnp.int32, (depth, width), 1) % HALF // months
    gram_ref[...] = jnp.zeros_like(gram_ref)

    def add_slot(slot):
        received = jnp.concatenate(
            [
                jnp.concatenate(
                    [
                        inbox[lat_device * tm_devices + tm, slot]
                        for lat_device in range(lat_devices)
                    ],
                    axis=0,
                )
                for tm in range(tm_devices)
            ],
            axis=1,
        )
        first = pl.multiple_of(slot * depth, 8)
        merged = None
        for part in range(share):
            basis = jnp.concatenate(
                [
                    legendre[part * per_share + g, pl.ds(first, depth), :].astype(jnp.bfloat16)
                    for g in range(per_share)
                ],
                axis=1,
            )
            product = jnp.dot(basis, received, preferred_element_type=jnp.float32)
            merged = product if part == 0 else jnp.where(share_of == part, product, merged)
        total = merged
        for part in range(1, share):
            total = total + pltpu.roll(merged, width - part * months, 1)
        coefficients = jnp.where(share_of == 0, total, 0.0).astype(jnp.bfloat16)
        gram_ref[...] += lax.dot_general(
            coefficients,
            coefficients,
            (((0,), (0,)), ((), ())),
            preferred_element_type=jnp.float32,
        )

    for phase, (low, top) in enumerate(phases):
        for first, last, count in runs:
            if count > low:

                @pl.loop(first * tm_devices, last * tm_devices)
                def _(source):
                    @pl.when(source != me)
                    def _():
                        exchange(phase, count, source, source).wait_recv()

        pl.loop(low, top)(add_slot)

    gram = None
    for part in range(2):
        across = jnp.concatenate(
            [
                gram_ref[pl.ds(tm * LANES + part * HALF, months), :]
                for tm in range(tm_devices)
            ],
            axis=0,
        )
        block = jnp.concatenate(
            [
                across[:, tm * LANES + part * HALF : tm * LANES + part * HALF + months]
                for tm in range(tm_devices)
            ],
            axis=1,
        )
        gram = block if gram is None else gram + block
    local_gram[...] = gram.reshape(pieces, PIECE, month_total)

    def owner(piece):
        return first_owner + piece * stride

    def send_part(piece, source):
        return pltpu.make_async_remote_copy(
            src_ref=local_gram.at[piece],
            dst_ref=parts.at[source],
            send_sem=part_send.at[piece],
            recv_sem=part_recv.at[source],
            device_id=coords(owner(piece)),
            device_id_type=MESH,
        )

    def send_sum(piece, target):
        return pltpu.make_async_remote_copy(
            src_ref=own_sum,
            dst_ref=full.at[piece],
            send_sem=sum_send.at[target],
            recv_sem=sum_recv.at[piece],
            device_id=coords(target),
            device_id_type=MESH,
        )

    @pl.loop(0, pieces)
    def _(piece):
        @pl.when(owner(piece) != me)
        def _():
            send_part(piece, me).start()

    is_owner = (
        (me >= first_owner)
        & (me < first_owner + pieces * stride)
        & (lax.rem(me - first_owner + device_total, stride) == 0)
    )
    my_piece = lax.rem(me - first_owner + device_total, device_total) // stride

    @pl.when(is_owner)
    def _():
        parts[me] = local_gram[my_piece]

        @pl.loop(1, device_total)
        def _(step):
            source = lax.rem(me + step, device_total)
            send_part(my_piece, source).wait_recv()

        total = lax.fori_loop(
            0,
            device_total,
            lambda source, value: value + parts[source],
            jnp.zeros((PIECE, month_total), jnp.float32),
        )
        own_sum[...] = total
        full[my_piece] = total

        @pl.loop(1, device_total)
        def _(step):
            send_sum(my_piece, lax.rem(me + step, device_total)).start()

    @pl.loop(0, pieces)
    def _(piece):
        @pl.when(owner(piece) != me)
        def _():
            send_sum(piece, me).wait_recv()

    gram = full[...].reshape(month_total, month_total)
    on_diagonal = lax.broadcasted_iota(jnp.int32, gram.shape, 0) == lax.broadcasted_iota(
        jnp.int32, gram.shape, 1
    )
    trace = jnp.sum(jnp.where(on_diagonal, gram, 0.0))
    mine = full[pl.ds(tm_me * (months // PIECE), months // PIECE)].reshape(months, month_total)
    out_ref[...] = month_total * mine / (trace + 1e-06)

    each_send(lambda copy: copy.wait_send())

    @pl.loop(0, pieces)
    def _(piece):
        @pl.when(owner(piece) != me)
        def _():
            send_part(piece, me).wait_send()

    @pl.when(is_owner)
    def _():
        @pl.loop(1, device_total)
        def _(step):
            send_sum(my_piece, lax.rem(me + step, device_total)).wait_send()


def solution(mesh):
    lat_devices = mesh.shape["lat"]
    tm_devices = mesh.shape["tm"]
    device_total = lat_devices * tm_devices
    slots = -(-(TRUNC + 1) // device_total)
    slot_rows = -(-slots // 8) * 8
    depth = -(-(TRUNC + 1) // 8) * 8

    def local(fields):
        rows, months, lon_count = fields.shape
        month_total = months * tm_devices
        lat_total = rows * lat_devices
        share = HALF // months
        high = rows // share
        pieces = month_total // PIECE
        width = tm_devices * LANES
        dims = (lat_devices, tm_devices, rows, months, lon_count, slots, slot_rows, depth)
        table = jnp.asarray(twiddle_table(device_total, slots, lon_count))
        starts = jnp.asarray(start_table(device_total, slots, slot_rows))
        lats = jnp.asarray(lat_table(lat_total, share))
        runs = needed_slots(lat_devices, device_total, slots, rows)
        phases = -(-slots // -(-slots // PHASES))
        hbm = pl.BlockSpec(memory_space=pl.ANY)
        vmem = pl.BlockSpec(memory_space=pltpu.VMEM)
        dma = pltpu.SemaphoreType.DMA
        return pl.pallas_call(
            functools.partial(kernel, dims, runs),
            out_shape=jax.ShapeDtypeStruct((months, month_total), jnp.float32),
            in_specs=[hbm, hbm, vmem, vmem],
            out_specs=vmem,
            scratch_shapes=[
                pltpu.VMEM((rows * months, lon_count), jnp.bfloat16),
                pltpu.VMEM(table.shape, jnp.bfloat16),
                pltpu.VMEM((GROUP * slots * high, LANES), jnp.float32),
                pltpu.VMEM((device_total, slots, high, LANES), jnp.bfloat16),
                pltpu.VMEM((device_total, slots, high, LANES), jnp.bfloat16),
                pltpu.VMEM((lat_total // LANES, slot_rows * depth, LANES), jnp.float32),
                pltpu.VMEM((width, width), jnp.float32),
                pltpu.VMEM((pieces, PIECE, month_total), jnp.float32),
                pltpu.VMEM((device_total, PIECE, month_total), jnp.float32),
                pltpu.VMEM((PIECE, month_total), jnp.float32),
                pltpu.VMEM((pieces, PIECE, month_total), jnp.float32),
                dma,
                dma((table.shape[0],)),
                dma((phases, device_total)),
                dma((phases, device_total)),
                dma((pieces,)),
                dma((device_total,)),
                dma((device_total,)),
                dma((pieces,)),
            ],
            compiler_params=pltpu.CompilerParams(
                collective_id=0, has_side_effects=True, vmem_limit_bytes=60 * 1024 * 1024
            ),
        )(fields.reshape(rows * months, lon_count), table, starts, lats)

    return jax.shard_map(
        local, mesh=mesh, in_specs=(P("lat", "tm", None),), out_specs=P("tm", None), check_vma=False
    )
```

```python
import functools
import math

import jax
import jax.numpy as jnp
import numpy as np
from jax import lax
from jax.experimental import pallas as pl
from jax.experimental.pallas import tpu as pltpu
from jax.sharding import PartitionSpec as P

TRUNC = 341
LANES = 128
HALF = 64
PIECE = 8
PHASES = 4
MESH = pl.DeviceIdType.MESH


def phase_bounds(slots):
    length = -(-slots // PHASES)
    return [(low, min(low + length, slots)) for low in range(0, slots, length)]


def twiddle_table(device_total, slots, lon_count):
    longitude = np.arange(lon_count)
    parts = []
    for low, top in phase_bounds(slots):
        device = np.arange(device_total)[:, None]
        wave = (np.arange(low, top)[None, :] * device_total + device).reshape(-1, 1)
        phase = 2.0 * math.pi * ((wave * longitude) % lon_count) / lon_count
        active = (wave <= TRUNC) / math.sqrt(lon_count)
        parts += [np.cos(phase) * active, -np.sin(phase) * active]
    return np.concatenate(parts).astype(np.float32).astype(jnp.bfloat16)


def start_table(device_total, slots, slot_rows):
    table = np.zeros((device_total, slot_rows), np.float64)
    for device in range(device_total):
        for slot in range(slot_rows):
            order = min(slot, slots - 1) * device_total + device
            table[device, slot] = 0.5 * (
                math.log(0.5)
                + math.lgamma(order + 1.5)
                - math.lgamma(1.5)
                - math.lgamma(order + 1.0)
            )
    table = np.broadcast_to(table[:, :, None], (device_total, slot_rows, LANES))
    return table.astype(np.float32)


def needed_slots(lat_devices, device_total, slots, rows):
    counts = []
    order = np.arange(slots * device_total)
    rise = np.array(
        [math.lgamma(m + 1.5) - math.lgamma(1.5) - math.lgamma(m + 1.0) for m in order]
    )
    for device in range(lat_devices):
        lat = device * rows + np.arange(rows)
        sine = np.sin(math.pi * (lat + 0.5) / (lat_devices * rows))
        start = 0.5 * (math.log(0.5) + rise[:, None]) + order[:, None] * np.log(sine)[None, :]
        used = (start > -70.5) & (order <= TRUNC)[:, None]
        used = used.reshape(slots, -1).any(axis=1)
        counts.append(int(np.max(np.nonzero(used)[0])) + 1 if used.any() else 0)
    runs = []
    for device, count in enumerate(counts):
        if runs and runs[-1][2] == count:
            runs[-1][1] = device + 1
        else:
            runs.append([device, device + 1, count])
    return tuple(tuple(run) for run in runs)


def lat_table(lat_total, share):
    lat = np.arange(lat_total).reshape(lat_total // share, share).T.reshape(-1)
    theta = math.pi * (lat + 0.5) / lat_total
    table = np.stack([np.cos(theta), np.log(np.sin(theta)), math.pi * np.sin(theta) / lat_total])
    return table.reshape(3, lat_total // LANES, LANES).astype(np.float32)


def kernel(
    dims,
    runs,
    x_hbm,
    table_hbm,
    start_ref,
    lat_ref,
    out_ref,
    x_ref,
    table_ref,
    spread,
    outbox,
    inbox,
    legendre,
    gram_ref,
    local_gram,
    parts,
    own_sum,
    full,
    x_sem,
    table_sem,
    send_sem,
    recv_sem,
    part_send,
    part_recv,
    sum_send,
    sum_recv,
):
    lat_devices, tm_devices, rows, months, lon_count, slots, slot_rows, depth = dims
    device_total = lat_devices * tm_devices
    share = HALF // months
    high = rows // share
    lat_total = lat_devices * rows
    lat_groups = lat_total // LANES
    month_total = months * tm_devices
    pieces = month_total // PIECE
    stride = device_total // 2 // pieces
    first_owner = device_total // 4
    lat_me = lax.axis_index("lat")
    tm_me = lax.axis_index("tm")
    me = lat_me * tm_devices + tm_me

    phases = phase_bounds(slots)

    def each_peer(act):
        def row(lat):
            for tm in range(tm_devices):
                act(lat, tm)

        pl.loop(lat_me + 1, lat_devices)(row)
        pl.loop(0, lat_me)(row)
        for tm in range(tm_devices):

            @pl.when(tm_me != tm)
            def _():
                act(lat_me, tm)

    x_copy = pltpu.make_async_copy(x_hbm, x_ref, x_sem)
    x_copy.start()

    def table_copy(phase):
        low, top = phases[phase]
        span = pl.ds(2 * device_total * low, 2 * device_total * (top - low))
        return pltpu.make_async_copy(table_hbm.at[span], table_ref.at[span], table_sem.at[phase])

    for phase in range(len(phases)):
        table_copy(phase).start()

    barrier = pltpu.get_barrier_semaphore()
    each_peer(
        lambda lat, tm: pl.semaphore_signal(
            barrier, inc=1, device_id=(lat, tm), device_id_type=MESH
        )
    )

    for first, last, count in runs:
        if count < slots:

            @pl.loop(first * tm_devices, last * tm_devices)
            def _(source):
                inbox[source, count:] = jnp.zeros((slots - count, high, LANES), jnp.bfloat16)

    def transform(phase):
        low, top = phases[phase]
        group_rows = device_total * (top - low)
        lower = lax.broadcasted_iota(jnp.int32, (group_rows, LANES), 1) < HALF
        table_copy(phase).wait()
        values = lax.dot_general(
            table_ref[2 * device_total * low : 2 * device_total * top],
            x_ref[...],
            (((1,), (1,)), ((), ())),
            preferred_element_type=jnp.float32,
        )
        for block in range(rows * months // LANES):
            cosine = values[:group_rows, block * LANES : (block + 1) * LANES]
            sine = values[group_rows:, block * LANES : (block + 1) * LANES]
            even = jnp.where(lower, cosine, pltpu.roll(sine, HALF, 1))
            odd = jnp.where(lower, pltpu.roll(cosine, HALF, 1), sine)
            spread[pl.ds(2 * block, group_rows, stride=high), :] = even
            spread[pl.ds(2 * block + 1, group_rows, stride=high), :] = odd
        packed = spread[: group_rows * high].astype(jnp.bfloat16)
        outbox[:, low:top] = packed.reshape(device_total, top - low, high, LANES)

    def exchange(phase, count, lat, tm, source):
        low, top = phases[phase]
        span = pl.ds(low, min(count, top) - low)
        target = lat * tm_devices + tm
        return pltpu.make_async_remote_copy(
            src_ref=outbox.at[target, span],
            dst_ref=inbox.at[source, span],
            send_sem=send_sem.at[phase, target],
            recv_sem=recv_sem.at[phase, source],
            device_id=(lat, tm),
            device_id_type=MESH,
        )

    def each_send(phase, act):
        for first, last, count in runs:
            if count > phases[phase][0]:

                @pl.when((lat_me >= first) & (lat_me < last))
                def _():
                    each_peer(lambda lat, tm: act(exchange(phase, count, lat, tm, me)))

    x_copy.wait()
    for phase in range(len(phases)):
        transform(phase)
        if phase == 0:
            pl.semaphore_wait(barrier, device_total - 1)
        each_send(phase, lambda copy: copy.start())

    inbox[me] = outbox[me]

    halves = slot_rows // 8
    sub = lax.broadcasted_iota(jnp.int32, (8, LANES), 0)
    slot_of = [sub + 8 * half for half in range(halves)]
    order_int = [slot * device_total + me for slot in slot_of]
    order = [value.astype(jnp.float32) for value in order_int]
    cosine_lat = [jnp.broadcast_to(lat_ref[0, pl.ds(g, 1), :], (8, LANES)) for g in range(lat_groups)]
    current = []
    scale = []
    for half in range(halves):
        factor = jnp.where(order_int[half] > 0, math.sqrt(2.0), 1.0)
        for g in range(lat_groups):
            log_start = (
                start_ref[me, pl.ds(8 * half, 8), :]
                + order[half] * jnp.broadcast_to(lat_ref[1, pl.ds(g, 1), :], (8, LANES))
            )
            taper = jnp.clip((log_start + 70.0) / 10.0, 0.0, 1.0)
            current.append(jnp.exp(jnp.maximum(log_start, -80.0)) * taper)
            scale.append(factor * jnp.broadcast_to(lat_ref[2, pl.ds(g, 1), :], (8, LANES)))

    def store(offset, values):
        for half in range(halves):
            keep = (order_int[half] + offset <= TRUNC) & (slot_of[half] < slots)
            for g in range(lat_groups):
                index = half * lat_groups + g
                value = jnp.where(keep, values[index] * scale[index], 0.0)
                legendre[g, pl.ds(8 * half * depth + offset, 8, stride=depth), :] = value

    store(0, current)

    def advance(offset, carry):
        now, before, backs = carry
        real = lax.convert_element_type(offset, jnp.float32)
        following = []
        next_backs = []
        for half in range(halves):
            degree = order[half] + real
            ratio = (4.0 * degree * degree - 1.0) / (real * (order[half] + degree))
            top = jnp.sqrt(ratio)
            next_backs.append(1.0 / top)
            for g in range(lat_groups):
                index = half * lat_groups + g
                following.append(
                    top * (cosine_lat[g] * now[index] - backs[half] * before[index])
                )
        store(offset, following)
        return following, now, next_backs

    zero = jnp.zeros((8, LANES), jnp.float32)
    lax.fori_loop(
        1,
        depth,
        advance,
        (current, [zero] * len(current), [zero] * halves),
        unroll=7,
    )

    per_share = lat_groups // share
    width = tm_devices * LANES
    share_of = lax.broadcasted_iota(jnp.int32, (depth, width), 1) % HALF // months
    gram_ref[...] = jnp.zeros_like(gram_ref)

    def add_slot(slot):
        received = jnp.concatenate(
            [
                jnp.concatenate(
                    [
                        inbox[lat_device * tm_devices + tm, slot]
                        for lat_device in range(lat_devices)
                    ],
                    axis=0,
                )
                for tm in range(tm_devices)
            ],
            axis=1,
        )
        first = pl.multiple_of(slot * depth, 8)
        merged = None
        for part in range(share):
            basis = jnp.concatenate(
                [
                    legendre[part * per_share + g, pl.ds(first, depth), :].astype(jnp.bfloat16)
                    for g in range(per_share)
                ],
                axis=1,
            )
            product = jnp.dot(basis, received, preferred_element_type=jnp.float32)
            merged = product if part == 0 else jnp.where(share_of == part, product, merged)
        total = merged
        for part in range(1, share):
            total = total + pltpu.roll(merged, width - part * months, 1)
        coefficients = jnp.where(share_of == 0, total, 0.0).astype(jnp.bfloat16)
        gram_ref[...] += lax.dot_general(
            coefficients,
            coefficients,
            (((0,), (0,)), ((), ())),
            preferred_element_type=jnp.float32,
        )

    for phase, (low, top) in enumerate(phases):
        for first, last, count in runs:
            if count > low:

                @pl.loop(first, last)
                def _(lat):
                    for tm in range(tm_devices):
                        source = lat * tm_devices + tm

                        @pl.when(source != me)
                        def _():
                            exchange(phase, count, lat, tm, source).wait_recv()

        pl.loop(low, top)(add_slot)

    gram = None
    for part in range(2):
        across = jnp.concatenate(
            [
                gram_ref[pl.ds(tm * LANES + part * HALF, months), :]
                for tm in range(tm_devices)
            ],
            axis=0,
        )
        block = jnp.concatenate(
            [
                across[:, tm * LANES + part * HALF : tm * LANES + part * HALF + months]
                for tm in range(tm_devices)
            ],
            axis=1,
        )
        gram = block if gram is None else gram + block
    local_gram[...] = gram.reshape(pieces, PIECE, month_total)

    lat_step = stride // tm_devices
    first_lat = first_owner // tm_devices

    def owner(piece):
        return first_lat + piece * lat_step

    def send_part(piece, source):
        return pltpu.make_async_remote_copy(
            src_ref=local_gram.at[piece],
            dst_ref=parts.at[source],
            send_sem=part_send.at[piece],
            recv_sem=part_recv.at[source],
            device_id=(owner(piece), 0),
            device_id_type=MESH,
        )

    def send_sum(piece, lat, tm):
        return pltpu.make_async_remote_copy(
            src_ref=own_sum,
            dst_ref=full.at[piece],
            send_sem=sum_send.at[lat * tm_devices + tm],
            recv_sem=sum_recv.at[piece],
            device_id=(lat, tm),
            device_id_type=MESH,
        )

    def not_mine(piece):
        return (owner(piece) != lat_me) | (tm_me != 0)

    @pl.loop(0, pieces)
    def _(piece):
        @pl.when(not_mine(piece))
        def _():
            send_part(piece, me).start()

    for phase in range(len(phases)):
        each_send(phase, lambda copy: copy.wait_send())

    @pl.loop(0, pieces)
    def _(piece):
        @pl.when((owner(piece) == lat_me) & (tm_me == 0))
        def _():
            parts[me] = local_gram[piece]
            each_peer(lambda lat, tm: send_part(piece, lat * tm_devices + tm).wait_recv())
            total = jnp.sum(parts[...], axis=0)
            own_sum[...] = total
            full[piece] = total
            each_peer(lambda lat, tm: send_sum(piece, lat, tm).start())

    @pl.loop(0, pieces)
    def _(piece):
        @pl.when(not_mine(piece))
        def _():
            send_sum(piece, lat_me, tm_me).wait_recv()

    gram = full[...].reshape(month_total, month_total)
    on_diagonal = lax.broadcasted_iota(jnp.int32, gram.shape, 0) == lax.broadcasted_iota(
        jnp.int32, gram.shape, 1
    )
    trace = jnp.sum(jnp.where(on_diagonal, gram, 0.0))
    mine = full[pl.ds(tm_me * (months // PIECE), months // PIECE)].reshape(months, month_total)
    out_ref[...] = month_total * mine / (trace + 1e-06)

    @pl.loop(0, pieces)
    def _(piece):
        @pl.when(not_mine(piece))
        def _():
            send_part(piece, me).wait_send()

        @pl.when((owner(piece) == lat_me) & (tm_me == 0))
        def _():
            each_peer(lambda lat, tm: send_sum(piece, lat, tm).wait_send())


def solution(mesh):
    lat_devices = mesh.shape["lat"]
    tm_devices = mesh.shape["tm"]
    device_total = lat_devices * tm_devices
    slots = -(-(TRUNC + 1) // device_total)
    slot_rows = -(-slots // 8) * 8
    depth = -(-(TRUNC + 1) // 8) * 8

    def local(fields):
        rows, months, lon_count = fields.shape
        month_total = months * tm_devices
        lat_total = rows * lat_devices
        share = HALF // months
        high = rows // share
        pieces = month_total // PIECE
        width = tm_devices * LANES
        dims = (lat_devices, tm_devices, rows, months, lon_count, slots, slot_rows, depth)
        table = jnp.asarray(twiddle_table(device_total, slots, lon_count))
        starts = jnp.asarray(start_table(device_total, slots, slot_rows))
        lats = jnp.asarray(lat_table(lat_total, share))
        runs = needed_slots(lat_devices, device_total, slots, rows)
        phases = phase_bounds(slots)
        longest = max(top - low for low, top in phases)
        hbm = pl.BlockSpec(memory_space=pl.ANY)
        vmem = pl.BlockSpec(memory_space=pltpu.VMEM)
        dma = pltpu.SemaphoreType.DMA
        return pl.pallas_call(
            functools.partial(kernel, dims, runs),
            out_shape=jax.ShapeDtypeStruct((months, month_total), jnp.float32),
            in_specs=[hbm, hbm, vmem, vmem],
            out_specs=vmem,
            scratch_shapes=[
                pltpu.VMEM((rows * months, lon_count), jnp.bfloat16),
                pltpu.VMEM(table.shape, jnp.bfloat16),
                pltpu.VMEM((device_total * longest * high, LANES), jnp.float32),
                pltpu.VMEM((device_total, slots, high, LANES), jnp.bfloat16),
                pltpu.VMEM((device_total, slots, high, LANES), jnp.bfloat16),
                pltpu.VMEM((lat_total // LANES, slot_rows * depth, LANES), jnp.float32),
                pltpu.VMEM((width, width), jnp.float32),
                pltpu.VMEM((pieces, PIECE, month_total), jnp.float32),
                pltpu.VMEM((device_total, PIECE, month_total), jnp.float32),
                pltpu.VMEM((PIECE, month_total), jnp.float32),
                pltpu.VMEM((pieces, PIECE, month_total), jnp.float32),
                dma,
                dma((len(phases),)),
                dma((len(phases), device_total)),
                dma((len(phases), device_total)),
                dma((pieces,)),
                dma((device_total,)),
                dma((device_total,)),
                dma((pieces,)),
            ],
            compiler_params=pltpu.CompilerParams(
                collective_id=0, has_side_effects=True, vmem_limit_bytes=60 * 1024 * 1024
            ),
        )(fields.reshape(rows * months, lon_count), table, starts, lats)

    return jax.shard_map(
        local, mesh=mesh, in_specs=(P("lat", "tm", None),), out_specs=P("tm", None), check_vma=False
    )
```

```python
import functools
import math

import jax
import jax.numpy as jnp
import numpy as np
from jax import lax
from jax.experimental import pallas as pl
from jax.experimental.pallas import tpu as pltpu
from jax.sharding import PartitionSpec as P

TRUNC = 341
LANES = 128
HALF = 64
PIECE = 8
PHASES = 3
MESH = pl.DeviceIdType.MESH


def phase_bounds(slots):
    length = -(-slots // PHASES)
    return [(low, min(low + length, slots)) for low in range(0, slots, length)]


def twiddle_table(device_total, slots, lon_count):
    longitude = np.arange(lon_count)
    parts = []
    for low, top in phase_bounds(slots):
        device = np.arange(device_total)[:, None]
        wave = (np.arange(low, top)[None, :] * device_total + device).reshape(-1, 1)
        phase = 2.0 * math.pi * ((wave * longitude) % lon_count) / lon_count
        active = (wave <= TRUNC) / math.sqrt(lon_count)
        parts += [np.cos(phase) * active, -np.sin(phase) * active]
    return np.concatenate(parts).astype(np.float32).astype(jnp.bfloat16)


def start_table(device_total, slots, slot_rows):
    table = np.zeros((device_total, slot_rows), np.float64)
    for device in range(device_total):
        for slot in range(slot_rows):
            order = min(slot, slots - 1) * device_total + device
            table[device, slot] = 0.5 * (
                math.log(0.5)
                + math.lgamma(order + 1.5)
                - math.lgamma(1.5)
                - math.lgamma(order + 1.0)
            )
    table = np.broadcast_to(table[:, :, None], (device_total, slot_rows, LANES))
    return table.astype(np.float32)


def needed_slots(lat_devices, device_total, slots, rows):
    counts = []
    order = np.arange(slots * device_total)
    rise = np.array(
        [math.lgamma(m + 1.5) - math.lgamma(1.5) - math.lgamma(m + 1.0) for m in order]
    )
    for device in range(lat_devices):
        lat = device * rows + np.arange(rows)
        sine = np.sin(math.pi * (lat + 0.5) / (lat_devices * rows))
        start = 0.5 * (math.log(0.5) + rise[:, None]) + order[:, None] * np.log(sine)[None, :]
        used = (start > -70.5) & (order <= TRUNC)[:, None]
        used = used.reshape(slots, -1).any(axis=1)
        counts.append(int(np.max(np.nonzero(used)[0])) + 1 if used.any() else 0)
    runs = []
    for device, count in enumerate(counts):
        if runs and runs[-1][2] == count:
            runs[-1][1] = device + 1
        else:
            runs.append([device, device + 1, count])
    return tuple(tuple(run) for run in runs)


def lat_table(lat_total, share):
    lat = np.arange(lat_total).reshape(lat_total // share, share).T.reshape(-1)
    theta = math.pi * (lat + 0.5) / lat_total
    table = np.stack([np.cos(theta), np.log(np.sin(theta)), math.pi * np.sin(theta) / lat_total])
    return table.reshape(3, lat_total // LANES, LANES).astype(np.float32)


def kernel(
    dims,
    runs,
    x_hbm,
    table_hbm,
    start_ref,
    lat_ref,
    out_ref,
    x_ref,
    table_ref,
    spread,
    outbox,
    inbox,
    legendre,
    gram_ref,
    local_gram,
    parts,
    own_sum,
    full,
    x_sem,
    table_sem,
    send_sem,
    recv_sem,
    part_send,
    part_recv,
    sum_send,
    sum_recv,
):
    lat_devices, tm_devices, rows, months, lon_count, slots, slot_rows, depth = dims
    device_total = lat_devices * tm_devices
    share = HALF // months
    high = rows // share
    lat_total = lat_devices * rows
    lat_groups = lat_total // LANES
    month_total = months * tm_devices
    pieces = month_total // PIECE
    stride = device_total // 2 // pieces
    first_owner = device_total // 4
    lat_me = lax.axis_index("lat")
    tm_me = lax.axis_index("tm")
    me = lat_me * tm_devices + tm_me

    phases = phase_bounds(slots)

    def each_peer(act):
        def row(lat):
            for tm in range(tm_devices):
                act(lat, tm)

        pl.loop(lat_me + 1, lat_devices)(row)
        pl.loop(0, lat_me)(row)
        for tm in range(tm_devices):

            @pl.when(tm_me != tm)
            def _():
                act(lat_me, tm)

    x_copy = pltpu.make_async_copy(x_hbm, x_ref, x_sem)
    x_copy.start()

    def table_copy(phase):
        low, top = phases[phase]
        span = pl.ds(2 * device_total * low, 2 * device_total * (top - low))
        return pltpu.make_async_copy(table_hbm.at[span], table_ref.at[span], table_sem.at[phase])

    for phase in range(len(phases)):
        table_copy(phase).start()

    barrier = pltpu.get_barrier_semaphore()
    each_peer(
        lambda lat, tm: pl.semaphore_signal(
            barrier, inc=1, device_id=(lat, tm), device_id_type=MESH
        )
    )

    for first, last, count in runs:
        if count < slots:

            @pl.loop(first * tm_devices, last * tm_devices)
            def _(source):
                inbox[source, count:] = jnp.zeros((slots - count, high, LANES), jnp.bfloat16)

    def transform(phase):
        low, top = phases[phase]
        group_rows = device_total * (top - low)
        lower = lax.broadcasted_iota(jnp.int32, (group_rows, LANES), 1) < HALF
        table_copy(phase).wait()
        values = lax.dot_general(
            table_ref[2 * device_total * low : 2 * device_total * top],
            x_ref[...],
            (((1,), (1,)), ((), ())),
            preferred_element_type=jnp.float32,
        )
        for block in range(rows * months // LANES):
            cosine = values[:group_rows, block * LANES : (block + 1) * LANES]
            sine = values[group_rows:, block * LANES : (block + 1) * LANES]
            even = jnp.where(lower, cosine, pltpu.roll(sine, HALF, 1))
            odd = jnp.where(lower, pltpu.roll(cosine, HALF, 1), sine)
            spread[pl.ds(2 * block, group_rows, stride=high), :] = even
            spread[pl.ds(2 * block + 1, group_rows, stride=high), :] = odd
        packed = spread[: group_rows * high].astype(jnp.bfloat16)
        outbox[:, low:top] = packed.reshape(device_total, top - low, high, LANES)

    def exchange(phase, count, lat, tm, source):
        low, top = phases[phase]
        span = pl.ds(low, min(count, top) - low)
        target = lat * tm_devices + tm
        return pltpu.make_async_remote_copy(
            src_ref=outbox.at[target, span],
            dst_ref=inbox.at[source, span],
            send_sem=send_sem.at[phase, target],
            recv_sem=recv_sem.at[phase, source],
            device_id=(lat, tm),
            device_id_type=MESH,
        )

    def each_send(phase, act):
        for first, last, count in runs:
            if count > phases[phase][0]:

                @pl.when((lat_me >= first) & (lat_me < last))
                def _():
                    each_peer(lambda lat, tm: act(exchange(phase, count, lat, tm, me)))

    x_copy.wait()
    for phase in range(len(phases)):
        transform(phase)
        if phase == 0:
            pl.semaphore_wait(barrier, device_total - 1)
        each_send(phase, lambda copy: copy.start())

    inbox[me] = outbox[me]

    halves = slot_rows // 8
    sub = lax.broadcasted_iota(jnp.int32, (8, LANES), 0)
    slot_of = [sub + 8 * half for half in range(halves)]
    order_int = [slot * device_total + me for slot in slot_of]
    order = [value.astype(jnp.float32) for value in order_int]
    cosine_lat = [jnp.broadcast_to(lat_ref[0, pl.ds(g, 1), :], (8, LANES)) for g in range(lat_groups)]
    current = []
    scale = []
    for half in range(halves):
        factor = jnp.where(order_int[half] > 0, math.sqrt(2.0), 1.0)
        for g in range(lat_groups):
            log_start = (
                start_ref[me, pl.ds(8 * half, 8), :]
                + order[half] * jnp.broadcast_to(lat_ref[1, pl.ds(g, 1), :], (8, LANES))
            )
            taper = jnp.clip((log_start + 70.0) / 10.0, 0.0, 1.0)
            current.append(jnp.exp(jnp.maximum(log_start, -80.0)) * taper)
            scale.append(factor * jnp.broadcast_to(lat_ref[2, pl.ds(g, 1), :], (8, LANES)))

    def store(offset, values):
        for half in range(halves):
            keep = (order_int[half] + offset <= TRUNC) & (slot_of[half] < slots)
            for g in range(lat_groups):
                index = half * lat_groups + g
                value = jnp.where(keep, values[index] * scale[index], 0.0)
                legendre[g, pl.ds(8 * half * depth + offset, 8, stride=depth), :] = value

    store(0, current)

    def advance(offset, carry):
        now, before, backs = carry
        real = lax.convert_element_type(offset, jnp.float32)
        following = []
        next_backs = []
        for half in range(halves):
            degree = order[half] + real
            ratio = (4.0 * degree * degree - 1.0) / (real * (order[half] + degree))
            top = jnp.sqrt(ratio)
            next_backs.append(1.0 / top)
            for g in range(lat_groups):
                index = half * lat_groups + g
                following.append(
                    top * (cosine_lat[g] * now[index] - backs[half] * before[index])
                )
        store(offset, following)
        return following, now, next_backs

    zero = jnp.zeros((8, LANES), jnp.float32)
    lax.fori_loop(
        1,
        depth,
        advance,
        (current, [zero] * len(current), [zero] * halves),
        unroll=7,
    )

    per_share = lat_groups // share
    width = tm_devices * LANES
    share_of = lax.broadcasted_iota(jnp.int32, (depth, width), 1) % HALF // months
    gram_ref[...] = jnp.zeros_like(gram_ref)

    def add_slot(slot):
        received = jnp.concatenate(
            [
                jnp.concatenate(
                    [
                        inbox[lat_device * tm_devices + tm, slot]
                        for lat_device in range(lat_devices)
                    ],
                    axis=0,
                )
                for tm in range(tm_devices)
            ],
            axis=1,
        )
        first = pl.multiple_of(slot * depth, 8)
        merged = None
        for part in range(share):
            basis = jnp.concatenate(
                [
                    legendre[part * per_share + g, pl.ds(first, depth), :].astype(jnp.bfloat16)
                    for g in range(per_share)
                ],
                axis=1,
            )
            product = jnp.dot(basis, received, preferred_element_type=jnp.float32)
            merged = product if part == 0 else jnp.where(share_of == part, product, merged)
        total = merged
        for part in range(1, share):
            total = total + pltpu.roll(merged, width - part * months, 1)
        coefficients = jnp.where(share_of == 0, total, 0.0).astype(jnp.bfloat16)
        gram_ref[...] += lax.dot_general(
            coefficients,
            coefficients,
            (((0,), (0,)), ((), ())),
            preferred_element_type=jnp.float32,
        )

    for phase, (low, top) in enumerate(phases):
        for first, last, count in runs:
            if count > low:

                @pl.loop(first, last)
                def _(lat):
                    for tm in range(tm_devices):
                        source = lat * tm_devices + tm

                        @pl.when(source != me)
                        def _():
                            exchange(phase, count, lat, tm, source).wait_recv()

        pl.loop(low, top)(add_slot)

    gram = None
    for part in range(2):
        across = jnp.concatenate(
            [
                gram_ref[pl.ds(tm * LANES + part * HALF, months), :]
                for tm in range(tm_devices)
            ],
            axis=0,
        )
        block = jnp.concatenate(
            [
                across[:, tm * LANES + part * HALF : tm * LANES + part * HALF + months]
                for tm in range(tm_devices)
            ],
            axis=1,
        )
        gram = block if gram is None else gram + block
    local_gram[...] = gram.reshape(pieces, PIECE, month_total)

    lat_step = stride // tm_devices
    first_lat = first_owner // tm_devices

    def owner(piece):
        return first_lat + piece * lat_step

    def send_part(piece, source):
        return pltpu.make_async_remote_copy(
            src_ref=local_gram.at[piece],
            dst_ref=parts.at[source],
            send_sem=part_send.at[piece],
            recv_sem=part_recv.at[source],
            device_id=(owner(piece), 0),
            device_id_type=MESH,
        )

    def send_sum(piece, lat, tm):
        return pltpu.make_async_remote_copy(
            src_ref=own_sum,
            dst_ref=full.at[piece],
            send_sem=sum_send.at[lat * tm_devices + tm],
            recv_sem=sum_recv.at[piece],
            device_id=(lat, tm),
            device_id_type=MESH,
        )

    def not_mine(piece):
        return (owner(piece) != lat_me) | (tm_me != 0)

    @pl.loop(0, pieces)
    def _(piece):
        @pl.when(not_mine(piece))
        def _():
            send_part(piece, me).start()

    for phase in range(len(phases)):
        each_send(phase, lambda copy: copy.wait_send())

    @pl.loop(0, pieces)
    def _(piece):
        @pl.when((owner(piece) == lat_me) & (tm_me == 0))
        def _():
            parts[me] = local_gram[piece]
            each_peer(lambda lat, tm: send_part(piece, lat * tm_devices + tm).wait_recv())
            total = jnp.sum(parts[...], axis=0)
            own_sum[...] = total
            full[piece] = total
            each_peer(lambda lat, tm: send_sum(piece, lat, tm).start())

    @pl.loop(0, pieces)
    def _(piece):
        @pl.when(not_mine(piece))
        def _():
            send_sum(piece, lat_me, tm_me).wait_recv()

    gram = full[...].reshape(month_total, month_total)
    on_diagonal = lax.broadcasted_iota(jnp.int32, gram.shape, 0) == lax.broadcasted_iota(
        jnp.int32, gram.shape, 1
    )
    trace = jnp.sum(jnp.where(on_diagonal, gram, 0.0))
    mine = full[pl.ds(tm_me * (months // PIECE), months // PIECE)].reshape(months, month_total)
    out_ref[...] = month_total * mine / (trace + 1e-06)

    @pl.loop(0, pieces)
    def _(piece):
        @pl.when(not_mine(piece))
        def _():
            send_part(piece, me).wait_send()

        @pl.when((owner(piece) == lat_me) & (tm_me == 0))
        def _():
            each_peer(lambda lat, tm: send_sum(piece, lat, tm).wait_send())


def solution(mesh):
    lat_devices = mesh.shape["lat"]
    tm_devices = mesh.shape["tm"]
    device_total = lat_devices * tm_devices
    slots = -(-(TRUNC + 1) // device_total)
    slot_rows = -(-slots // 8) * 8
    depth = -(-(TRUNC + 1) // 8) * 8

    def local(fields):
        rows, months, lon_count = fields.shape
        month_total = months * tm_devices
        lat_total = rows * lat_devices
        share = HALF // months
        high = rows // share
        pieces = month_total // PIECE
        width = tm_devices * LANES
        dims = (lat_devices, tm_devices, rows, months, lon_count, slots, slot_rows, depth)
        table = jnp.asarray(twiddle_table(device_total, slots, lon_count))
        starts = jnp.asarray(start_table(device_total, slots, slot_rows))
        lats = jnp.asarray(lat_table(lat_total, share))
        runs = needed_slots(lat_devices, device_total, slots, rows)
        phases = phase_bounds(slots)
        longest = max(top - low for low, top in phases)
        hbm = pl.BlockSpec(memory_space=pl.ANY)
        vmem = pl.BlockSpec(memory_space=pltpu.VMEM)
        dma = pltpu.SemaphoreType.DMA
        return pl.pallas_call(
            functools.partial(kernel, dims, runs),
            out_shape=jax.ShapeDtypeStruct((months, month_total), jnp.float32),
            in_specs=[hbm, hbm, vmem, vmem],
            out_specs=vmem,
            scratch_shapes=[
                pltpu.VMEM((rows * months, lon_count), jnp.bfloat16),
                pltpu.VMEM(table.shape, jnp.bfloat16),
                pltpu.VMEM((device_total * longest * high, LANES), jnp.float32),
                pltpu.VMEM((device_total, slots, high, LANES), jnp.bfloat16),
                pltpu.VMEM((device_total, slots, high, LANES), jnp.bfloat16),
                pltpu.VMEM((lat_total // LANES, slot_rows * depth, LANES), jnp.float32),
                pltpu.VMEM((width, width), jnp.float32),
                pltpu.VMEM((pieces, PIECE, month_total), jnp.float32),
                pltpu.VMEM((device_total, PIECE, month_total), jnp.float32),
                pltpu.VMEM((PIECE, month_total), jnp.float32),
                pltpu.VMEM((pieces, PIECE, month_total), jnp.float32),
                dma,
                dma((len(phases),)),
                dma((len(phases), device_total)),
                dma((len(phases), device_total)),
                dma((pieces,)),
                dma((device_total,)),
                dma((device_total,)),
                dma((pieces,)),
            ],
            compiler_params=pltpu.CompilerParams(
                collective_id=0, has_side_effects=True, vmem_limit_bytes=60 * 1024 * 1024
            ),
        )(fields.reshape(rows * months, lon_count), table, starts, lats)

    return jax.shard_map(
        local, mesh=mesh, in_specs=(P("lat", "tm", None),), out_specs=P("tm", None), check_vma=False
    )
```
